64 devices in a mesh: rep: 8 (over x, y, core), dp: 8 (over z).
Axes of the slice: x: 2, y: 2, z: 8, core: 2. Of those that a mesh axis runs over, the one named last changes fastest.
The devices are a block of a 4x4x8 slice.
Arguments:
- x: bfloat16 [64, 4096, 512], P(('rep', 'dp')), parts along dimension 0
- dy: bfloat16 [64, 4096, 512], P(('rep', 'dp')), parts along dimension 0
- w_gate: bfloat16 [2, 512, 1792], replicated
- w_up: bfloat16 [2, 512, 1792], replicated
- w_down: bfloat16 [2, 1792, 512], replicated
- m_w_gate: float32 [2, 512, 1792], P(None, 'dp')
- m_w_up: float32 [2, 512, 1792], P(None, 'dp')
- m_w_down: float32 [2, 1792, 512], P(None, 'dp')
- v_w_gate: float32 [2, 512, 1792], P(None, 'dp')
- v_w_up: float32 [2, 512, 1792], P(None, 'dp')
- v_w_down: float32 [2, 1792, 512], P(None, 'dp')
Outputs:
- output 1: bfloat16 [16, 512, 1792], P('rep'), parts along dimension 0
- output 2: bfloat16 [16, 512, 1792], P('rep'), parts along dimension 0
- output 3: bfloat16 [16, 1792, 512], P('rep'), parts along dimension 0
- output 4: float32 [16, 512, 1792], P('rep', 'dp'), parts along dimension 0
- output 5: float32 [16, 512, 1792], P('rep', 'dp'), parts along dimension 0
- output 6: float32 [16, 1792, 512], P('rep', 'dp'), parts along dimension 0
- output 7: float32 [16, 512, 1792], P('rep', 'dp'), parts along dimension 0
- output 8: float32 [16, 512, 1792], P('rep', 'dp'), parts along dimension 0
- output 9: float32 [16, 1792, 512], P('rep', 'dp'), parts along dimension 0
There are 8 independent parts. The reference program is written for one: setup_inputs(seed, part) draws one part's arguments, and reference() takes and returns one part's arrays. A program takes and returns all parts, laid end to end along the dimension named above; an argument that names none is the same for every part.
All inputs are finite; a program needn't handle non-finite values.
Results may differ from the reference program's by a relative error of at most 0.0204.
Values are sent between devices in bfloat16 or wider.
A program may use at most 768 MiB of HBM per device.

```python
import jax
import jax.numpy as jnp
from jax import lax

SEQUENCES = 8
TOKENS = 4096
D = 512
FF = 1792
LAYERS = 2
NAMES = ("w_gate", "w_up", "w_down")
SHAPES = {"w_gate": (LAYERS, D, FF), "w_up": (LAYERS, D, FF), "w_down": (LAYERS, FF, D)}


def bump(key, n, height):
    away = (jnp.arange(n, dtype=jnp.int32) - jax.random.randint(key, (), 0, n, jnp.int32)) % n
    return jnp.where(away < n // 8, height, 1.0)


def together(key, own, strength):
    shared = jax.random.normal(key, own.shape[1:], jnp.float32)
    return (own + strength * shared) * lax.rsqrt(1 + strength * strength)


def setup_inputs(seed: int = 0, part: int = 0) -> dict:
    kx, kdy, ka, kb, kz, kf, kh, kl, *keys = jax.random.split(jax.random.key(seed), 8 + 3 * len(NAMES))
    kx, kdy, ka, kb = (jax.random.fold_in(k, part) for k in (kx, kdy, ka, kb))
    kw, km, kv = (keys[i::3] for i in range(3))
    shape = (SEQUENCES, TOKENS, D)
    much_x, much_dy = jax.random.uniform(kz, (2,), jnp.float32, 0.0, 1.0)
    loud = 2.0 ** jax.random.uniform(jax.random.fold_in(kz, 1), (), jnp.float32, -1.0, 2.0)
    layers = 2.0 ** jax.random.uniform(kl, (LAYERS, 1, 1), jnp.float32, -1.0, 1.0)
    x = together(ka, jax.random.normal(kx, shape, jnp.float32), much_x) * bump(kf, D, 4.0)
    dy = together(kb, jax.random.normal(kdy, shape, jnp.float32), much_dy)
    drawn = {"x": x.astype(jnp.bfloat16), "dy": (loud * dy * (SEQUENCES * TOKENS) ** -0.5).astype(jnp.bfloat16)}
    for key, name in zip(kw, NAMES, strict=True):
        w = jax.random.normal(key, SHAPES[name], jnp.float32) * SHAPES[name][1] ** -0.5
        drawn[name] = (w * {"w_gate": 1.0, "w_up": bump(kh, FF, 4.0), "w_down": layers}[name]).astype(jnp.bfloat16)
    for key, name in zip(km, NAMES, strict=True):
        drawn[f"m_{name}"] = 0.1 * jax.random.normal(key, SHAPES[name], jnp.float32)
    for key, name in zip(kv, NAMES, strict=True):
        drawn[f"v_{name}"] = jax.random.uniform(key, SHAPES[name], jnp.float32, 0.005, 0.015)
    return drawn


def matmul(a, w):
    return jnp.dot(a, w, preferred_element_type=jnp.float32).astype(jnp.bfloat16)


def normed(h):
    wide = h.astype(jnp.float32)
    scale = lax.rsqrt(jnp.mean(wide**2, -1, keepdims=True) + 1e-6)
    return (wide * scale).astype(jnp.bfloat16)


def layer(h, w):
    a = normed(h)
    gate = jnp.dot(a, w["w_gate"], preferred_element_type=jnp.float32)
    up = jnp.dot(a, w["w_up"], preferred_element_type=jnp.float32)
    return h + matmul((jax.nn.silu(gate) * up).astype(jnp.bfloat16), w["w_down"])


def adamw(w, m, v, g):
    m = 0.9 * m + 0.1 * g
    v = 0.95 * v + 0.05 * g * g
    step = m * lax.rsqrt(v + 1e-8) + 0.1 * w
    return (w - 0.02 * step).astype(jnp.bfloat16), m, v


def stack(weights, h):
    return lax.scan(lambda h, w: (layer(h, w), None), h, weights)[0]


def reference(x, dy, w_gate, w_up, w_down, m_w_gate, m_w_up, m_w_down, v_w_gate, v_w_up, v_w_down):
    weights = dict(zip(NAMES, (w_gate, w_up, w_down), strict=True))

    def take(so_far, sequence):
        h, by_y = sequence
        _, back = jax.vjp(lambda w: stack(w, h), weights)
        return jax.tree.map(lambda total, term: total + term.astype(jnp.float32), so_far, back(by_y)[0]), None

    none_yet = {name: jnp.zeros(w.shape, jnp.float32) for name, w in weights.items()}
    by_weights, _ = lax.scan(take, none_yet, (x, dy))
    gradients = [by_weights[name].astype(jnp.bfloat16).astype(jnp.float32) for name in NAMES]
    new = [
        adamw(w.astype(jnp.float32), m, v, g)
        for w, m, v, g in zip((w_gate, w_up, w_down), (m_w_gate, m_w_up, m_w_down), (v_w_gate, v_w_up, v_w_down), gradients, strict=True)
    ]
    return tuple(one[which] for which in range(3) for one in new)
```

```python
import functools

import jax
import jax.numpy as jnp
from jax import lax
from jax.experimental import pallas as pl
from jax.experimental.pallas import tpu as pltpu
from jax.sharding import PartitionSpec as P

BF = jnp.bfloat16
F32 = jnp.float32
TILE = 512
TOK = 1024
COLS = 256
VMEM_LIMIT = 67043328


def mm(a, b):
    return jnp.dot(a, b, preferred_element_type=F32)


def mm_nt(a, b):
    return lax.dot_general(a, b, (((1,), (1,)), ((), ())), preferred_element_type=F32)


def normed(h):
    wide = h.astype(F32)
    scale = lax.rsqrt(jnp.mean(wide * wide, -1, keepdims=True) + 1e-6)
    return (wide * scale).astype(BF)


def forward_kernel(x_ref, dy_ref, wg_ref, wu_ref, wd_ref, a1_ref, a1t_ref, a2_ref, a2t_ref, h_ref, dyt_ref):
    x = x_ref[0]
    a = normed(x)
    a1_ref[...] = a
    a1t_ref[...] = a.T
    dyt_ref[...] = dy_ref[0].T
    total = None
    for j in range(wg_ref.shape[2] // COLS):
        cols = slice(j * COLS, (j + 1) * COLS)
        gate = mm(a, wg_ref[0, :, cols])
        up = mm(a, wu_ref[0, :, cols])
        act = (gate * jax.nn.sigmoid(gate) * up).astype(BF)
        part = mm(act, wd_ref[0, cols, :])
        total = part if total is None else total + part
    h = (x.astype(F32) + total.astype(BF).astype(F32)).astype(BF)
    h_ref[...] = h
    a2 = normed(h)
    a2_ref[...] = a2
    a2t_ref[...] = a2.T


def forward(x, dy, wg, wu, wd):
    _, tokens, d = x.shape
    ff = wg.shape[2]
    row = pl.BlockSpec((1, TILE, d), lambda i: (0, i, 0))
    out = pl.BlockSpec((TILE, d), lambda i: (i, 0))
    out_t = pl.BlockSpec((d, TILE), lambda i: (0, i))
    w_in = pl.BlockSpec((1, d, ff), lambda i: (0, 0, 0))
    w_out = pl.BlockSpec((1, ff, d), lambda i: (0, 0, 0))
    straight, turned = jax.ShapeDtypeStruct((tokens, d), BF), jax.ShapeDtypeStruct((d, tokens), BF)
    return pl.pallas_call(
        forward_kernel,
        grid=(tokens // TILE,),
        in_specs=[row, row, w_in, w_in, w_out],
        out_specs=[out, out_t, out, out_t, out, out_t],
        out_shape=[straight, turned, straight, turned, straight, turned],
        compiler_params=pltpu.CompilerParams(vmem_limit_bytes=VMEM_LIMIT, dimension_semantics=("arbitrary",)),
        name="forward",
    )(x, dy, wg, wu, wd)


def tile_grads(top, layer, j, t, refs):
    A, AT, D, DT, DA, WG, WU, WD, GU, DWT = refs
    rows = slice(t * TOK, (t + 1) * TOK)
    cols = pl.ds(pl.multiple_of(j * COLS, COLS), COLS)
    wg, wu = WG[layer, :, cols], WU[layer, :, cols]
    a, dy = A[rows, :], D[rows, :]
    gate, up = mm(a, wg), mm(a, wu)
    dact = mm_nt(dy, WD[layer, cols, :]).astype(BF).astype(F32)
    sig = jax.nn.sigmoid(gate)
    silu = gate * sig
    act = (silu * up).astype(BF)
    dup = (dact * silu).astype(BF)
    dgate = (dact * up * (sig + silu * (1.0 - sig))).astype(BF)
    at, dt = AT[:, rows], DT[:, rows]
    n, rows_of, _ = GU.shape
    half = rows_of // 2
    dwt = mm(dt, act)
    dwg = mm(at, dgate).reshape(n, half, COLS)
    dwu = mm(at, dup).reshape(n, half, COLS)
    if t == 0:
        DWT[...] = dwt
        GU[:, :half, :] = dwg
        GU[:, half:, :] = dwu
    else:
        DWT[...] += dwt
        GU[:, :half, :] += dwg
        GU[:, half:, :] += dwu
    if top:
        da = mm_nt(dgate, wg) + mm_nt(dup, wu)

        @pl.when(j == 0)
        def _():
            DA[rows, :] = da

        @pl.when(j > 0)
        def _():
            DA[rows, :] += da


def through_norm(t, A_, D, DT, H, DA):
    rows = slice(t * TILE, (t + 1) * TILE)
    h = H[rows, :].astype(F32)
    s = lax.rsqrt(jnp.mean(h * h, -1, keepdims=True) + 1e-6)
    da = DA[rows, :].astype(BF).astype(F32)
    dh = da * s - h * (s * s * s * jnp.mean(da * h, -1, keepdims=True))
    dh = (D[rows, :].astype(F32) + dh.astype(BF).astype(F32)).astype(BF)
    D[rows, :] = dh
    DT[:, rows] = dh.T


def grads_kernel(
    n, dy_h, a1_h, a1t_h, a2_h, a2t_h, h_h, dyt_h, wg_h, wu_h, wd_h,
    gu_o, gd_o,
    A, AT, D, DT, H, DA, WG, WU, WD, GU, GUB, DWT, DW, DWB, load, wsem, hsem, osem,
):
    tokens, d = A.shape
    nt = tokens // TOK
    ff = WG.shape[2]
    nj = ff // COLS

    def tile_loads(t, a_h, at_h, with_dy):
        rows = slice(t * TOK, (t + 1) * TOK)
        pairs = [(a_h.at[rows, :], A.at[rows, :]), (at_h.at[:, rows], AT.at[:, rows])]
        if with_dy:
            pairs += [(dy_h.at[0, rows, :], D.at[rows, :]), (dyt_h.at[:, rows], DT.at[:, rows])]
        return [pltpu.make_async_copy(s, o, load.at[t, i]) for i, (s, o) in enumerate(pairs)]

    weights = [
        pltpu.make_async_copy(s.at[l], o.at[l], wsem.at[l, i])
        for l in (1, 0) for i, (s, o) in enumerate(((wg_h, WG), (wu_h, WU), (wd_h, WD)))
    ]
    for c in weights[:3]:
        c.start()
    for t in range(nt):
        for c in tile_loads(t, a2_h, a2t_h, True):
            c.start()
    hcopy = pltpu.make_async_copy(h_h, H, hsem)
    hcopy.start()
    for c in weights[3:]:
        c.start()
    for c in weights[:3]:
        c.wait()

    refs = (A, AT, D, DT, DA, WG, WU, WD, GU, DWT)

    def finish(layer, j):
        @pl.when((j > 0) if layer else (j >= 0))
        def _():
            pltpu.make_async_copy(GUB, gu_o.at[0, :, 0], osem.at[0]).wait()
        GUB[...] = GU[...].astype(BF)
        pltpu.make_async_copy(GUB, gu_o.at[layer, :, j], osem.at[0]).start()
        DW[pl.ds(pl.multiple_of(j * COLS, COLS), COLS), :] = DWT[...].T

    def top_block(j, carry):
        for t in range(nt):
            @pl.when(j == 0)
            def _():
                for c in tile_loads(t, a2_h, a2t_h, True):
                    c.wait()
            tile_grads(True, 1, j, t, refs)

            @pl.when(j == nj - 1)
            def _():
                for c in tile_loads(t, a1_h, a1t_h, False):
                    c.start()
        finish(1, j)
        return carry

    lax.fori_loop(0, nj, top_block, 0)
    DWB[...] = DW[...].astype(BF)
    pltpu.make_async_copy(DWB, gd_o.at[1], osem.at[1]).start()
    hcopy.wait()
    for c in weights[3:]:
        c.wait()
    for t in range(tokens // TILE):
        through_norm(t, A, D, DT, H, DA)

    def low_block(j, carry):
        for t in range(nt):
            @pl.when(j == 0)
            def _():
                for c in tile_loads(t, a1_h, a1t_h, False):
                    c.wait()
            tile_grads(False, 0, j, t, refs)
        finish(0, j)
        return carry

    lax.fori_loop(0, nj, low_block, 0)
    pltpu.make_async_copy(DWB, gd_o.at[1], osem.at[1]).wait()
    DWB[...] = DW[...].astype(BF)
    pltpu.make_async_copy(DWB, gd_o.at[0], osem.at[1]).start()
    pltpu.make_async_copy(GUB, gu_o.at[0, :, 0], osem.at[0]).wait()
    pltpu.make_async_copy(DWB, gd_o.at[0], osem.at[1]).wait()


def grads(n, dy, a1, a1t, a2, a2t, h, dyt, wg, wu, wd):
    tokens, d = a1.shape
    layers, _, ff = wg.shape
    nj, nt = ff // COLS, tokens // TOK
    block = (n, 2 * d // n, COLS)
    any_ = pl.BlockSpec(memory_space=pl.ANY)
    return pl.pallas_call(
        functools.partial(grads_kernel, n),
        in_specs=[any_] * 10,
        out_specs=[any_] * 2,
        out_shape=[jax.ShapeDtypeStruct((layers, n, nj, *block[1:]), BF), jax.ShapeDtypeStruct((layers, ff, d), BF)],
        scratch_shapes=[
            pltpu.VMEM((tokens, d), BF), pltpu.VMEM((d, tokens), BF), pltpu.VMEM((tokens, d), BF), pltpu.VMEM((d, tokens), BF),
            pltpu.VMEM((tokens, d), BF), pltpu.VMEM((tokens, d), F32),
            pltpu.VMEM((layers, d, ff), BF), pltpu.VMEM((layers, d, ff), BF), pltpu.VMEM((layers, ff, d), BF),
            pltpu.VMEM(block, F32), pltpu.VMEM(block, BF), pltpu.VMEM((d, COLS), F32), pltpu.VMEM((ff, d), F32), pltpu.VMEM((ff, d), BF),
            pltpu.SemaphoreType.DMA((nt, 4)), pltpu.SemaphoreType.DMA((2, 3)), pltpu.SemaphoreType.DMA, pltpu.SemaphoreType.DMA((2,)),
        ],
        compiler_params=pltpu.CompilerParams(vmem_limit_bytes=VMEM_LIMIT),
        name="grads",
    )(dy, a1, a1t, a2, a2t, h, dyt, wg, wu, wd)


def adamw(w, m, v, g):
    m = 0.9 * m + 0.1 * g
    v = 0.95 * v + 0.05 * g * g
    step = m * lax.rsqrt(v + 1e-8) + 0.1 * w
    return (w - 0.02 * step).astype(BF), m, v


def solution(mesh):
    n = mesh.shape["dp"]

    def step(x, dy, wg, wu, wd, mg, mu, md, vg, vu, vd):
        layers, d, ff = wg.shape
        nj, half = ff // COLS, d // n
        a1, a1t, a2, a2t, h, dyt = forward(x, dy, wg, wu, wd)
        gu, gd = grads(n, dy, a1, a1t, a2, a2t, h, dyt, wg, wu, wd)
        out = []
        me = lax.axis_index("dp")
        new = {}
        for l in range(layers - 1, -1, -1):
            gul = lax.psum_scatter(gu[l], "dp", scatter_dimension=0, tiled=True)
            gul = gul.reshape(nj, 2, half, COLS).transpose(1, 2, 0, 3).reshape(2, half, ff).astype(F32)
            gdl = lax.psum_scatter(gd[l], "dp", scatter_dimension=0, tiled=True).astype(F32)
            for k, (w, m, v, g) in enumerate(((wg, mg, vg, gul[0]), (wu, mu, vu, gul[1]), (wd, md, vd, gdl))):
                mine = lax.dynamic_slice_in_dim(w[l], me * g.shape[0], g.shape[0], 0).astype(F32)
                nw, nm, nv = adamw(mine, m[l], v[l], g)
                new[l, k] = (lax.all_gather(nw, "dp", axis=0, tiled=True), nm, nv)
        return tuple(jnp.stack([new[l, k][which] for l in range(layers)]) for which in range(3) for k in range(3))

    data, whole, own = P(("rep", "dp"), None, None), P(), P(None, "dp", None)
    return jax.shard_map(
        step, mesh=mesh, in_specs=(data,) * 2 + (whole,) * 3 + (own,) * 6,
        out_specs=(P("rep", None, None),) * 3 + (P("rep", "dp", None),) * 6, check_vma=False,
    )
```

```python
import functools

import jax
import jax.numpy as jnp
from jax import lax
from jax.experimental import pallas as pl
from jax.experimental.pallas import tpu as pltpu
from jax.sharding import PartitionSpec as P

BF = jnp.bfloat16
F32 = jnp.float32
TILE = 512
TOK = 1024
COLS = 256
WIDE = 256
SLOTS = 3
MESH = pl.DeviceIdType.MESH
VMEM_LIMIT = 67043328


def mm(a, b):
    return jnp.dot(a, b, preferred_element_type=F32)


def mm_nt(a, b):
    return lax.dot_general(a, b, (((1,), (1,)), ((), ())), preferred_element_type=F32)


def normed(h):
    wide = h.astype(F32)
    scale = lax.rsqrt(jnp.mean(wide * wide, -1, keepdims=True) + 1e-6)
    return (wide * scale).astype(BF)


def forward_kernel(x_ref, dy_ref, wg_ref, wu_ref, wd_ref, a1_ref, a1t_ref, a2_ref, a2t_ref, h_ref, dyt_ref):
    x = x_ref[0]
    a = normed(x)
    a1_ref[...] = a
    a1t_ref[...] = a.T
    dyt_ref[...] = dy_ref[0].T
    total = None
    for j in range(wg_ref.shape[2] // COLS):
        cols = slice(j * COLS, (j + 1) * COLS)
        gate = mm(a, wg_ref[0, :, cols])
        up = mm(a, wu_ref[0, :, cols])
        act = (gate * jax.nn.sigmoid(gate) * up).astype(BF)
        part = mm(act, wd_ref[0, cols, :])
        total = part if total is None else total + part
    h = (x.astype(F32) + total.astype(BF).astype(F32)).astype(BF)
    h_ref[...] = h
    a2 = normed(h)
    a2_ref[...] = a2
    a2t_ref[...] = a2.T


def forward(x, dy, wg, wu, wd):
    _, tokens, d = x.shape
    ff = wg.shape[2]
    row = pl.BlockSpec((1, TILE, d), lambda i: (0, i, 0))
    out = pl.BlockSpec((TILE, d), lambda i: (i, 0))
    out_t = pl.BlockSpec((d, TILE), lambda i: (0, i))
    w_in = pl.BlockSpec((1, d, ff), lambda i: (0, 0, 0))
    w_out = pl.BlockSpec((1, ff, d), lambda i: (0, 0, 0))
    straight, turned = jax.ShapeDtypeStruct((tokens, d), BF), jax.ShapeDtypeStruct((d, tokens), BF)
    return pl.pallas_call(
        forward_kernel,
        grid=(tokens // TILE,),
        in_specs=[row, row, w_in, w_in, w_out],
        out_specs=[out, out_t, out, out_t, out, out_t],
        out_shape=[straight, turned, straight, turned, straight, turned],
        compiler_params=pltpu.CompilerParams(vmem_limit_bytes=VMEM_LIMIT, dimension_semantics=("arbitrary",)),
        name="forward",
    )(x, dy, wg, wu, wd)


def tile_grads(top, layer, j, t, slot, refs):
    A, AT, D, DT, S, WG, WU, WD, GU, DWT = refs
    rows = slice(t * TOK, (t + 1) * TOK)
    cols = pl.ds(pl.multiple_of(j * COLS, COLS), COLS)
    wg, wu = WG[layer, :, cols], WU[layer, :, cols]
    a, dy = A[rows, :], D[rows, :]
    gate, up = mm(a, wg), mm(a, wu)
    dact = mm_nt(dy, WD[layer, cols, :]).astype(BF).astype(F32)
    sig = jax.nn.sigmoid(gate)
    silu = gate * sig
    act = (silu * up).astype(BF)
    dup = (dact * silu).astype(BF)
    dgate = (dact * up * (sig + silu * (1.0 - sig))).astype(BF)
    at, dt = AT[:, rows], DT[:, rows]
    _, n, rows_of, _ = GU.shape
    half = rows_of // 2
    dwt = mm(dt, act)
    dwg = mm(at, dgate).reshape(n, half, COLS)
    dwu = mm(at, dup).reshape(n, half, COLS)
    if t == 0:
        DWT[...] = dwt
        GU[slot, :, :half, :] = dwg
        GU[slot, :, half:, :] = dwu
    else:
        DWT[...] += dwt
        GU[slot, :, :half, :] += dwg
        GU[slot, :, half:, :] += dwu
    if top:
        da = mm_nt(dgate, wg) + mm_nt(dup, wu)

        S[rows, :] += da


def through_norm(rows, A, D, DT, S):
    h = A[rows, :].astype(F32)
    s = lax.rsqrt(jnp.mean(h * h, -1, keepdims=True) + 1e-6)
    da = S[rows, :].astype(BF).astype(F32)
    dh = da * s - h * (s * s * s * jnp.mean(da * h, -1, keepdims=True))
    dh = (D[rows, :].astype(F32) + dh.astype(BF).astype(F32)).astype(BF)
    D[rows, :] = dh
    DT[:, rows] = dh.T


def adamw(w, m, v, g):
    m = 0.9 * m + 0.1 * g
    v = 0.95 * v + 0.05 * g * g
    step = m * lax.rsqrt(v + 1e-8) + 0.1 * w
    return (w - 0.02 * step).astype(BF), m, v


class Ring:
    def __init__(self, n, me, got, sems):
        self.n, self.me, self.hops = n, me, n // 2
        self.to = (lax.rem(me + n - 1, n), lax.rem(me + 1, n))
        self.got = got
        self.sum_out, self.sum_in, self.new_out, self.new_in = sems

    def owner(self, way, distance):
        return lax.rem(self.me + (self.n - distance if way == 0 else distance), self.n)

    def part(self, way, half_only):
        rows = self.got.shape[2]
        if not half_only:
            return slice(0, rows)
        return slice(0, rows // 2) if way == 0 else slice(rows // 2, rows)

    def sum_copy(self, way, step):
        part = self.part(way, step == 0)
        source = self.got.at[way, self.hops - 1, part] if step == 0 else self.got.at[way, step - 1]
        return pltpu.make_async_remote_copy(
            source, self.got.at[way, step, part], self.sum_out.at[way, step], self.sum_in.at[way, step],
            device_id={"dp": self.to[way]}, device_id_type=MESH,
        )

    def new_copy(self, way, step, new):
        part = self.part(way, step == self.hops - 1)
        block = new.at[self.owner(1 - way, step), part]
        return pltpu.make_async_remote_copy(
            block, block, self.new_out.at[way, step], self.new_in.at[way, step],
            device_id={"dp": self.to[way]}, device_id_type=MESH,
        )

    def arrived(self, way, step, new):
        part = self.part(way, step == self.hops - 1)
        block = new.at[self.owner(1 - way, step + 1), part]
        return pltpu.make_async_remote_copy(
            block, block, self.new_out.at[way, step], self.new_in.at[way, step],
            device_id={"dp": self.to[way]}, device_id_type=MESH,
        )

    def sum_step(self, step, local):
        for way in (0, 1):
            if step:
                before = self.sum_copy(way, step - 1)
                before.wait_send()
                before.wait_recv()
        for way in (0, 1):
            term = local(self.owner(way, self.hops - step))
            if step == 0:
                self.got[way, self.hops - 1, self.part(way, True)] = term[self.part(way, True)].astype(BF)
            elif step == 1:
                mine, other = self.part(way, True), self.part(1 - way, True)
                got = self.got[way, 0, mine].astype(F32)
                self.got[way, 0, mine] = (got + term[mine]).astype(BF)
                self.got[way, 0, other] = term[other].astype(BF)
            else:
                self.got[way, step - 1] = (self.got[way, step - 1].astype(F32) + term).astype(BF)
        for way in (0, 1):
            self.sum_copy(way, step).start()

    def total(self, local):
        for way in (0, 1):
            before = self.sum_copy(way, self.hops - 1)
            before.wait_send()
            before.wait_recv()
        total = local(self.me) + self.got[0, self.hops - 1].astype(F32) + self.got[1, self.hops - 1].astype(F32)
        return total.astype(BF).astype(F32)

    def new_step(self, step, new):
        for way in (0, 1):
            if step:
                self.new_copy(way, step - 1, new).wait_send()
                self.arrived(way, step - 1, new).wait_recv()
        if step < self.hops:
            for way in (0, 1):
                self.new_copy(way, step, new).start()


def grads_kernel(
    n, dy_h, a1_h, a1t_h, a2_h, a2t_h, h_h, dyt_h, wg_h, wu_h, wd_h, mg_h, mu_h, md_h, vg_h, vu_h, vd_h,
    wg_o, wu_o, wd_o, mg_o, mu_o, md_o, vg_o, vu_o, vd_o,
    A, AT, D, DT, S, WG, WU, WD, GU, DWT, NEW, NEWD, GOT, GOTD, MV, MVD,
    load, wsem, hsem, ring_sem, ringd_sem, mv_in, mv_out, mvd_in, mvd_out, out_sem, outd_sem,
):
    me = lax.axis_index("dp")
    left, right = lax.rem(me + n - 1, n), lax.rem(me + 1, n)
    barrier = pltpu.get_barrier_semaphore()
    for neighbour in (left, right):
        pl.semaphore_signal(barrier, inc=1, device_id={"dp": neighbour}, device_id_type=MESH)

    tokens, d = A.shape
    nt = tokens // TOK
    ff = WG.shape[2]
    nj = ff // COLS
    half, down = d // n, ff // n
    hops = n // 2
    streams = d // WIDE

    def tile_loads(t, a_h, at_h, with_dy):
        rows = slice(t * TOK, (t + 1) * TOK)
        pairs = [(a_h.at[rows, :], A.at[rows, :]), (at_h.at[:, rows], AT.at[:, rows])]
        if with_dy:
            pairs += [(dy_h.at[0, rows, :], D.at[rows, :]), (dyt_h.at[:, rows], DT.at[:, rows])]
        return [pltpu.make_async_copy(s, o, load.at[t, i]) for i, (s, o) in enumerate(pairs)]

    def h_load(t):
        rows = slice(t * TOK, (t + 1) * TOK)
        return pltpu.make_async_copy(h_h.at[rows, :], A.at[rows, :], hsem.at[t])

    weights = [
        pltpu.make_async_copy(s.at[l], o.at[l], wsem.at[l, i])
        for l in (1, 0) for i, (s, o) in enumerate(((wg_h, WG), (wu_h, WU), (wd_h, WD)))
    ]
    for c in weights[:3]:
        c.start()
    for t in range(nt):
        for c in tile_loads(t, a2_h, a2t_h, True):
            c.start()
    for c in weights[3:]:
        c.start()
    S[:tokens, :] = jnp.zeros((tokens, d), F32)
    for c in weights[:3]:
        c.wait()
    pl.semaphore_wait(barrier, 2)

    refs = (A, AT, D, DT, S, WG, WU, WD, GU, DWT)

    def gate_up(c, op, step):
        slot, layer, j = lax.rem(c, SLOTS), 1 - c // nj, lax.rem(c, nj)
        ring = Ring(n, me, GOT.at[slot], [ring_sem.at[k, slot] for k in range(4)])
        new = NEW.at[c]
        cols = pl.ds(pl.multiple_of(j * COLS, COLS), COLS)
        place = lax.rem(c, 2)

        def local(device):
            return GU[slot, device]

        def moments(m_g, m_u, v_g, v_u):
            return [
                (m_g.at[layer, :, cols], MV.at[place, 0, :half]), (m_u.at[layer, :, cols], MV.at[place, 0, half:]),
                (v_g.at[layer, :, cols], MV.at[place, 1, :half]), (v_u.at[layer, :, cols], MV.at[place, 1, half:]),
            ]

        fetch = lambda: [pltpu.make_async_copy(a, b, mv_in.at[place, i]) for i, (a, b) in enumerate(moments(mg_h, mu_h, vg_h, vu_h))]
        keep = lambda: [pltpu.make_async_copy(b, a, mv_out.at[place, i]) for i, (a, b) in enumerate(moments(mg_o, mu_o, vg_o, vu_o))]
        write = lambda: [
            pltpu.make_async_copy(new.at[:, :half], wg_o.at[layer, :, :, cols], out_sem.at[place, 0]),
            pltpu.make_async_copy(new.at[:, half:], wu_o.at[layer, :, :, cols], out_sem.at[place, 1]),
        ]
        if op == "sum":
            if step == hops // 2:
                @pl.when(c >= 2)
                def _():
                    for copy in keep():
                        copy.wait()
                for copy in fetch():
                    copy.start()
            ring.sum_step(step, local)
        elif op == "update":
            for copy in fetch():
                copy.wait()
            g = ring.total(local)
            own = pl.ds(pl.multiple_of(me * half, half), half)
            for i, w in enumerate((WG, WU)):
                rows = slice(i * half, (i + 1) * half)
                nw, m, v = adamw(w[layer, own, cols].astype(F32), MV[place, 0, rows], MV[place, 1, rows], g[rows])
                MV[place, 0, rows] = m
                MV[place, 1, rows] = v
                NEW[c, me, rows] = nw
            ring.new_step(0, new)
            for copy in keep():
                copy.start()
        else:
            ring.new_step(step, new)
            if step == hops:
                @pl.when(c >= 2)
                def _():
                    for copy in write():
                        copy.wait()
                for copy in write():
                    copy.start()

    def down_block(layer, k, op, step):
        ring = Ring(n, me, GOTD.at[k], [ringd_sem.at[i, k] for i in range(4)])
        new = NEWD.at[layer, k]
        cols = slice(k * WIDE, (k + 1) * WIDE)

        def local(device):
            return S[pl.ds(pl.multiple_of(layer * tokens + device * down, 32), down), cols]

        fetch = lambda: [pltpu.make_async_copy(s.at[layer, :, cols], MVD.at[k, i], mvd_in.at[k, i]) for i, s in enumerate((md_h, vd_h))]
        keep = lambda: [pltpu.make_async_copy(MVD.at[k, i], o.at[layer, :, cols], mvd_out.at[k, i]) for i, o in enumerate((md_o, vd_o))]
        write = lambda: pltpu.make_async_copy(new, wd_o.at[layer, :, :, cols], outd_sem.at[k])
        if op == "sum":
            if step == hops // 2:
                @pl.when(layer == 0)
                def _():
                    for copy in keep():
                        copy.wait()
                for copy in fetch():
                    copy.start()
            ring.sum_step(step, local)
        elif op == "update":
            for copy in fetch():
                copy.wait()
            g = ring.total(local)
            own = pl.ds(pl.multiple_of(me * down, 32), down)
            nw, m, v = adamw(WD[layer, own, cols].astype(F32), MVD[k, 0], MVD[k, 1], g)
            MVD[k, 0] = m
            MVD[k, 1] = v
            NEWD[layer, k, me] = nw
            ring.new_step(0, new)
            for copy in keep():
                copy.start()
        else:
            ring.new_step(step, new)
            if step == hops:
                @pl.when(layer == 0)
                def _():
                    write().wait()
                write().start()

    steps = [("sum", s, 2 * s) for s in range(hops)] + [("update", 0, 2 * hops)]
    steps += [("new", s, 2 * hops + 1 + 2 * s) for s in range(1, hops + 1)]

    def tick(i, t, with_down):
        for op, step, after in steps:
            ago, at_tick = divmod(after, nt)
            if at_tick == t:
                c = i - 1 - ago

                @pl.when((c >= 0) & (c < 2 * nj))
                def _(c=c, op=op, step=step):
                    gate_up(c, op, step)
        if with_down:
            for k in range(streams):
                for op, step, after in steps:
                    ago, at_tick = divmod(after + 1 + 2 * k, nt)
                    if at_tick == t:
                        ready = i - ago

                        @pl.when((ready == nj) | (ready == 2 * nj))
                        def _(ready=ready, op=op, step=step, k=k):
                            down_block(2 - ready // nj, k, op, step)

    def finish(layer, j):
        S[pl.ds(pl.multiple_of(layer * tokens + j * COLS, COLS), COLS), :] = DWT[...].T

    def top_block(j, carry):
        for t in range(nt):
            tick(j, t, False)

            @pl.when(j == 0)
            def _():
                for c in tile_loads(t, a2_h, a2t_h, True):
                    c.wait()
            tile_grads(True, 1, j, t, lax.rem(j, SLOTS), refs)

            @pl.when(j == nj - 1)
            def _():
                h_load(t).start()
                tile_loads(t, a1_h, a1t_h, False)[1].start()
        finish(1, j)
        return carry

    lax.fori_loop(0, nj, top_block, 0)
    for c in weights[3:]:
        c.wait()
    for t in range(nt):
        h_load(t).wait()
        for u in range(TOK // TILE):
            through_norm(slice(t * TOK + u * TILE, t * TOK + (u + 1) * TILE), A, D, DT, S)
        tile_loads(t, a1_h, a1t_h, False)[0].start()

    def low_block(i, carry):
        for t in range(nt):
            tick(i, t, True)

            @pl.when(i < 2 * nj)
            def _():
                @pl.when(i == nj)
                def _():
                    for c in tile_loads(t, a1_h, a1t_h, False):
                        c.wait()
                tile_grads(False, 0, i - nj, t, lax.rem(i, SLOTS), refs)

        @pl.when(i < 2 * nj)
        def _():
            finish(0, i - nj)
        return carry

    last = 2 * nj + max(nt + steps[-1][2], 1 + 2 * (streams - 1) + steps[-1][2]) // nt
    lax.fori_loop(nj, last + 1, low_block, 0)

    for c in (2 * nj - 2, 2 * nj - 1):
        place, j = c % 2, c % nj
        cols = slice(j * COLS, (j + 1) * COLS)
        for i, o in enumerate((mg_o, mu_o, vg_o, vu_o)):
            pltpu.make_async_copy(MV.at[place, i // 2, (i % 2) * half : (i % 2 + 1) * half], o.at[0, :, cols], mv_out.at[place, i]).wait()
        for i, o in enumerate((wg_o, wu_o)):
            pltpu.make_async_copy(NEW.at[c, :, i * half : (i + 1) * half], o.at[0, :, :, cols], out_sem.at[place, i]).wait()
    for k in range(streams):
        cols = slice(k * WIDE, (k + 1) * WIDE)
        for i, o in enumerate((md_o, vd_o)):
            pltpu.make_async_copy(MVD.at[k, i], o.at[0, :, cols], mvd_out.at[k, i]).wait()
        pltpu.make_async_copy(NEWD.at[0, k], wd_o.at[0, :, :, cols], outd_sem.at[k]).wait()


def grads(n, *args):
    a1, wg, wd = args[1], args[7], args[9]
    tokens, d = a1.shape
    layers, _, ff = wg.shape
    nj, nt, hops, streams = ff // COLS, tokens // TOK, n // 2, d // WIDE
    half, down = d // n, ff // n
    any_ = pl.BlockSpec(memory_space=pl.ANY)
    dma = pltpu.SemaphoreType.DMA
    own = [jax.ShapeDtypeStruct((layers, half, ff), F32)] * 2 + [jax.ShapeDtypeStruct((layers, down, d), F32)]
    return pl.pallas_call(
        functools.partial(grads_kernel, n),
        in_specs=[any_] * len(args),
        out_specs=[any_] * 9,
        out_shape=[jax.ShapeDtypeStruct((layers, n, half, ff), BF)] * 2 + [jax.ShapeDtypeStruct((layers, n, down, d), BF)] + own + own,
        scratch_shapes=[
            pltpu.VMEM((tokens, d), BF), pltpu.VMEM((d, tokens), BF), pltpu.VMEM((tokens, d), BF), pltpu.VMEM((d, tokens), BF),
            pltpu.VMEM((tokens + ff, d), F32),
            pltpu.VMEM((layers, d, ff), BF), pltpu.VMEM((layers, d, ff), BF), pltpu.VMEM((layers, ff, d), BF),
            pltpu.VMEM((SLOTS, n, 2 * half, COLS), F32), pltpu.VMEM((d, COLS), F32),
            pltpu.VMEM((layers * nj, n, 2 * half, COLS), BF), pltpu.VMEM((layers, streams, n, down, WIDE), BF),
            pltpu.VMEM((SLOTS, 2, hops, 2 * half, COLS), BF),
            pltpu.VMEM((streams, 2, hops, down, WIDE), BF),
            pltpu.VMEM((2, 2, 2 * half, COLS), F32), pltpu.VMEM((streams, 2, down, WIDE), F32),
            dma((nt, 4)), dma((2, 3)), dma((nt,)), dma((4, SLOTS, 2, hops)), dma((4, streams, 2, hops)),
            dma((2, 4)), dma((2, 4)), dma((streams, 2)), dma((streams, 2)), dma((2, 2)), dma((streams,)),
        ],
        compiler_params=pltpu.CompilerParams(vmem_limit_bytes=VMEM_LIMIT, collective_id=0, has_side_effects=True),
        name="grads",
    )(*args)


def solution(mesh):
    n = mesh.shape["dp"]

    def step(x, dy, wg, wu, wd, mg, mu, md, vg, vu, vd):
        a1, a1t, a2, a2t, h, dyt = forward(x, dy, wg, wu, wd)
        out = grads(n, dy, a1, a1t, a2, a2t, h, dyt, wg, wu, wd, mg, mu, md, vg, vu, vd)
        return tuple(t.reshape(t.shape[0], -1, t.shape[-1]) for t in out)

    data, whole, own = P(("rep", "dp"), None, None), P(), P(None, "dp", None)
    return jax.shard_map(
        step, mesh=mesh, in_specs=(data,) * 2 + (whole,) * 3 + (own,) * 6,
        out_specs=(P("rep", None, None),) * 3 + (P("rep", "dp", None),) * 6, check_vma=False,
    )
```

```python
import functools

import jax
import jax.numpy as jnp
from jax import lax
from jax.experimental import pallas as pl
from jax.experimental.pallas import tpu as pltpu
from jax.sharding import PartitionSpec as P

BF = jnp.bfloat16
F32 = jnp.float32
TILE = 512
TOK = 1024
COLS = 256
WIDE = 256
DTOK = 256
PAUSE = 2
SLOTS = 3
MESH = pl.DeviceIdType.MESH
VMEM_LIMIT = 67043328


def mm(a, b):
    return jnp.dot(a, b, preferred_element_type=F32)


def mm_nt(a, b):
    return lax.dot_general(a, b, (((1,), (1,)), ((), ())), preferred_element_type=F32)


def normed(h):
    wide = h.astype(F32)
    scale = lax.rsqrt(jnp.mean(wide * wide, -1, keepdims=True) + 1e-6)
    return (wide * scale).astype(BF)


def forward_kernel(x_ref, dy_ref, wg_ref, wu_ref, wd_ref, a1_ref, a1t_ref, a2_ref, a2t_ref, h_ref, dyt_ref):
    x = x_ref[0]
    a = normed(x)
    a1_ref[...] = a
    a1t_ref[...] = a.T
    dyt_ref[...] = dy_ref[0].T
    total = None
    for j in range(wg_ref.shape[2] // COLS):
        cols = slice(j * COLS, (j + 1) * COLS)
        gate = mm(a, wg_ref[0, :, cols])
        up = mm(a, wu_ref[0, :, cols])
        act = (gate * jax.nn.sigmoid(gate) * up).astype(BF)
        part = mm(act, wd_ref[0, cols, :])
        total = part if total is None else total + part
    h = (x.astype(F32) + total.astype(BF).astype(F32)).astype(BF)
    h_ref[...] = h
    a2 = normed(h)
    a2_ref[...] = a2
    a2t_ref[...] = a2.T


def forward(x, dy, wg, wu, wd):
    _, tokens, d = x.shape
    ff = wg.shape[2]
    row = pl.BlockSpec((1, TILE, d), lambda i: (0, i, 0))
    out = pl.BlockSpec((TILE, d), lambda i: (i, 0))
    out_t = pl.BlockSpec((d, TILE), lambda i: (0, i))
    w_in = pl.BlockSpec((1, d, ff), lambda i: (0, 0, 0))
    w_out = pl.BlockSpec((1, ff, d), lambda i: (0, 0, 0))
    straight, turned = jax.ShapeDtypeStruct((tokens, d), BF), jax.ShapeDtypeStruct((d, tokens), BF)
    return pl.pallas_call(
        forward_kernel,
        grid=(tokens // TILE,),
        in_specs=[row, row, w_in, w_in, w_out],
        out_specs=[out, out_t, out, out_t, out, out_t],
        out_shape=[straight, turned, straight, turned, straight, turned],
        compiler_params=pltpu.CompilerParams(vmem_limit_bytes=VMEM_LIMIT, dimension_semantics=("arbitrary",)),
        name="forward",
    )(x, dy, wg, wu, wd)


def tile_grads(layer, j, t, slot, refs, keep=None):
    A, AT, D, DT, WG, WU, WD, GU, DWT = refs
    rows = slice(t * TOK, (t + 1) * TOK)
    cols = pl.ds(pl.multiple_of(j * COLS, COLS), COLS)
    wg, wu = WG[layer, :, cols], WU[layer, :, cols]
    a, dy = A[rows, :], D[rows, :]
    gate, up = mm(a, wg), mm(a, wu)
    dact = mm_nt(dy, WD[layer, cols, :]).astype(BF).astype(F32)
    sig = jax.nn.sigmoid(gate)
    silu = gate * sig
    act = (silu * up).astype(BF)
    dup = (dact * silu).astype(BF)
    dgate = (dact * up * (sig + silu * (1.0 - sig))).astype(BF)
    if keep is not None:
        keep[0] = dgate
        keep[1] = dup
    at, dt = AT[:, rows], DT[:, rows]
    _, n, rows_of, _ = GU.shape
    half = rows_of // 2
    dwt = mm(dt, act)
    dwg = mm(at, dgate).reshape(n, half, COLS)
    dwu = mm(at, dup).reshape(n, half, COLS)
    if t == 0:
        DWT[...] = dwt
        GU[slot, :, :half, :] = dwg
        GU[slot, :, half:, :] = dwu
    else:
        DWT[...] += dwt
        GU[slot, :, :half, :] += dwg
        GU[slot, :, half:, :] += dwu


def through_norm(rows, da, A, D, DT):
    h = A[rows, :].astype(F32)
    s = lax.rsqrt(jnp.mean(h * h, -1, keepdims=True) + 1e-6)
    da = da.astype(BF).astype(F32)
    dh = da * s - h * (s * s * s * jnp.mean(da * h, -1, keepdims=True))
    dh = (D[rows, :].astype(F32) + dh.astype(BF).astype(F32)).astype(BF)
    D[rows, :] = dh
    DT[:, rows] = dh.T


def adamw(w, m, v, g):
    m = 0.9 * m + 0.1 * g
    v = 0.95 * v + 0.05 * g * g
    step = m * lax.rsqrt(v + 1e-8) + 0.1 * w
    return (w - 0.02 * step).astype(BF), m, v


class Ring:
    def __init__(self, n, me, got, sems):
        self.n, self.me, self.hops = n, me, n // 2
        self.to = (lax.rem(me + n - 1, n), lax.rem(me + 1, n))
        self.got = got
        self.sum_out, self.sum_in, self.new_out, self.new_in = sems

    def owner(self, way, distance):
        return lax.rem(self.me + (self.n - distance if way == 0 else distance), self.n)

    def part(self, way, half_only):
        rows = self.got.shape[2]
        if not half_only:
            return slice(0, rows)
        return slice(0, rows // 2) if way == 0 else slice(rows // 2, rows)

    def sum_copy(self, way, step):
        part = self.part(way, step == 0)
        source = self.got.at[way, self.hops - 1, part] if step == 0 else self.got.at[way, step - 1]
        return pltpu.make_async_remote_copy(
            source, self.got.at[way, step, part], self.sum_out.at[way, step], self.sum_in.at[way, step],
            device_id={"dp": self.to[way]}, device_id_type=MESH,
        )

    def new_copy(self, way, step, new):
        part = self.part(way, step == self.hops - 1)
        block = new.at[self.owner(1 - way, step), part]
        return pltpu.make_async_remote_copy(
            block, block, self.new_out.at[way, step], self.new_in.at[way, step],
            device_id={"dp": self.to[way]}, device_id_type=MESH,
        )

    def arrived(self, way, step, new):
        part = self.part(way, step == self.hops - 1)
        block = new.at[self.owner(1 - way, step + 1), part]
        return pltpu.make_async_remote_copy(
            block, block, self.new_out.at[way, step], self.new_in.at[way, step],
            device_id={"dp": self.to[way]}, device_id_type=MESH,
        )

    def sum_step(self, step, local):
        for way in (0, 1):
            if step:
                before = self.sum_copy(way, step - 1)
                before.wait_send()
                before.wait_recv()
        for way in (0, 1):
            term = local(self.owner(way, self.hops - step))
            if step == 0:
                self.got[way, self.hops - 1, self.part(way, True)] = term[self.part(way, True)].astype(BF)
            elif step == 1:
                mine, other = self.part(way, True), self.part(1 - way, True)
                got = self.got[way, 0, mine].astype(F32)
                self.got[way, 0, mine] = (got + term[mine]).astype(BF)
                self.got[way, 0, other] = term[other].astype(BF)
            else:
                self.got[way, step - 1] = (self.got[way, step - 1].astype(F32) + term).astype(BF)
        for way in (0, 1):
            self.sum_copy(way, step).start()

    def total(self, local):
        for way in (0, 1):
            before = self.sum_copy(way, self.hops - 1)
            before.wait_send()
            before.wait_recv()
        total = local(self.me) + self.got[0, self.hops - 1].astype(F32) + self.got[1, self.hops - 1].astype(F32)
        return total.astype(BF).astype(F32)

    def new_step(self, step, new):
        for way in (0, 1):
            if step:
                self.new_copy(way, step - 1, new).wait_send()
                self.arrived(way, step - 1, new).wait_recv()
        if step < self.hops:
            for way in (0, 1):
                self.new_copy(way, step, new).start()


def grads_kernel(
    n, dy_h, a1_h, a1t_h, a2_h, a2t_h, h_h, dyt_h, wg_h, wu_h, wd_h, mg_h, mu_h, md_h, vg_h, vu_h, vd_h,
    wg_o, wu_o, wd_o, mg_o, mu_o, md_o, vg_o, vu_o, vd_o, dgu_h,
    A, AT, D, DT, S, WG, WU, WD, GU, DWT, NEW, NEWD, GOT, GOTD, MV, MVD, OUT, IN,
    load, wsem, hsem, ring_sem, ringd_sem, mv_in, mv_out, mvd_in, mvd_out, out_sem, outd_sem, dgu_out, dgu_in,
):
    me = lax.axis_index("dp")
    left, right = lax.rem(me + n - 1, n), lax.rem(me + 1, n)
    barrier = pltpu.get_barrier_semaphore()
    for neighbour in (left, right):
        pl.semaphore_signal(barrier, inc=1, device_id={"dp": neighbour}, device_id_type=MESH)

    tokens, d = A.shape
    nt = tokens // TOK
    ff = WG.shape[2]
    nj = ff // COLS
    half, down = d // n, ff // n
    hops = n // 2
    streams = d // WIDE

    def tile_loads(t, a_h, at_h, with_dy):
        rows = slice(t * TOK, (t + 1) * TOK)
        pairs = [(a_h.at[rows, :], A.at[rows, :]), (at_h.at[:, rows], AT.at[:, rows])]
        if with_dy:
            pairs += [(dy_h.at[0, rows, :], D.at[rows, :]), (dyt_h.at[:, rows], DT.at[:, rows])]
        return [pltpu.make_async_copy(s, o, load.at[t, i]) for i, (s, o) in enumerate(pairs)]

    def h_load(t):
        rows = slice(t * TOK, (t + 1) * TOK)
        return pltpu.make_async_copy(h_h.at[rows, :], A.at[rows, :], hsem.at[t])

    weights = [
        pltpu.make_async_copy(s.at[l], o.at[l], wsem.at[l, i])
        for l in (1, 0) for i, (s, o) in enumerate(((wg_h, WG), (wu_h, WU), (wd_h, WD)))
    ]
    for c in weights[:3]:
        c.start()
    for c in tile_loads(0, a2_h, a2t_h, True):
        c.start()
    for c in weights[:3]:
        c.wait()
    pl.semaphore_wait(barrier, 2)

    refs = (A, AT, D, DT, WG, WU, WD, GU, DWT)

    def gate_up(c, op, step):
        slot, layer, j = lax.rem(c, SLOTS), 1 - c // nj, lax.rem(c, nj)
        ring = Ring(n, me, GOT.at[slot], [ring_sem.at[k, slot] for k in range(4)])
        new = NEW.at[c]
        cols = pl.ds(pl.multiple_of(j * COLS, COLS), COLS)
        place = lax.rem(c, 2)

        def local(device):
            return GU[slot, device]

        def moments(m_g, m_u, v_g, v_u):
            return [
                (m_g.at[layer, :, cols], MV.at[place, 0, :half]), (m_u.at[layer, :, cols], MV.at[place, 0, half:]),
                (v_g.at[layer, :, cols], MV.at[place, 1, :half]), (v_u.at[layer, :, cols], MV.at[place, 1, half:]),
            ]

        fetch = lambda: [pltpu.make_async_copy(a, b, mv_in.at[place, i]) for i, (a, b) in enumerate(moments(mg_h, mu_h, vg_h, vu_h))]
        keep = lambda: [pltpu.make_async_copy(b, a, mv_out.at[place, i]) for i, (a, b) in enumerate(moments(mg_o, mu_o, vg_o, vu_o))]
        write = lambda: [
            pltpu.make_async_copy(new.at[:, :half], wg_o.at[layer, :, :, cols], out_sem.at[place, 0]),
            pltpu.make_async_copy(new.at[:, half:], wu_o.at[layer, :, :, cols], out_sem.at[place, 1]),
        ]
        if op == "sum":
            if step == hops // 2:
                @pl.when(c >= 2)
                def _():
                    for copy in keep():
                        copy.wait()
                for copy in fetch():
                    copy.start()
            ring.sum_step(step, local)
        elif op == "update":
            for copy in fetch():
                copy.wait()
            g = ring.total(local)
            own = pl.ds(pl.multiple_of(me * half, half), half)
            for i, w in enumerate((WG, WU)):
                rows = slice(i * half, (i + 1) * half)
                nw, m, v = adamw(w[layer, own, cols].astype(F32), MV[place, 0, rows], MV[place, 1, rows], g[rows])
                MV[place, 0, rows] = m
                MV[place, 1, rows] = v
                NEW[c, me, rows] = nw
            ring.new_step(0, new)
            for copy in keep():
                copy.start()
        else:
            ring.new_step(step, new)
            if step == hops:
                @pl.when(c >= 2)
                def _():
                    for copy in write():
                        copy.wait()
                for copy in write():
                    copy.start()

    def down_block(layer, k, op, step):
        ring = Ring(n, me, GOTD.at[k], [ringd_sem.at[i, k] for i in range(4)])
        new = NEWD.at[layer, k]
        cols = slice(k * WIDE, (k + 1) * WIDE)

        def local(device):
            return S[pl.ds(pl.multiple_of(layer * ff + device * down, 32), down), cols]

        fetch = lambda: [pltpu.make_async_copy(s.at[layer, :, cols], MVD.at[k, i], mvd_in.at[k, i]) for i, s in enumerate((md_h, vd_h))]
        keep = lambda: [pltpu.make_async_copy(MVD.at[k, i], o.at[layer, :, cols], mvd_out.at[k, i]) for i, o in enumerate((md_o, vd_o))]
        write = lambda: pltpu.make_async_copy(new, wd_o.at[layer, :, :, cols], outd_sem.at[k])
        if op == "sum":
            if step == hops // 2:
                @pl.when(layer == 0)
                def _():
                    for copy in keep():
                        copy.wait()
                for copy in fetch():
                    copy.start()
            ring.sum_step(step, local)
        elif op == "update":
            for copy in fetch():
                copy.wait()
            g = ring.total(local)
            own = pl.ds(pl.multiple_of(me * down, 32), down)
            nw, m, v = adamw(WD[layer, own, cols].astype(F32), MVD[k, 0], MVD[k, 1], g)
            MVD[k, 0] = m
            MVD[k, 1] = v
            NEWD[layer, k, me] = nw
            ring.new_step(0, new)
            for copy in keep():
                copy.start()
        else:
            ring.new_step(step, new)
            if step == hops:
                @pl.when(layer == 0)
                def _():
                    write().wait()
                write().start()

    steps = [("sum", s, 2 * s) for s in range(hops)] + [("update", 0, 2 * hops)]
    steps += [("new", s, 2 * hops + 1 + 2 * s) for s in range(1, hops + 1)]

    def tick(i, t, with_down):
        for op, step, after in steps:
            ago, at_tick = divmod(after, nt)
            if at_tick == t:
                x = i - 1 - ago

                @pl.when(((x >= 0) & (x < nj)) | ((x >= nj + PAUSE) & (x < 2 * nj + PAUSE)))
                def _(x=x, op=op, step=step):
                    gate_up(x - PAUSE * (x // (nj + PAUSE)), op, step)
        if with_down:
            for k in range(streams):
                for op, step, after in steps:
                    ago, at_tick = divmod(after + 1 + 2 * k, nt)
                    if at_tick == t:
                        ready = i - ago

                        @pl.when((ready == nj) | (ready == 2 * nj + PAUSE))
                        def _(ready=ready, op=op, step=step, k=k):
                            down_block(2 - ready // nj, k, op, step)

    def finish(layer, j):
        S[pl.ds(pl.multiple_of(layer * ff + j * COLS, COLS), COLS), :] = DWT[...].T

    def dgu_write(j, t):
        rows = slice(t * TOK, (t + 1) * TOK)
        cols = pl.ds(pl.multiple_of(j * COLS, COLS), COLS)
        return [pltpu.make_async_copy(OUT.at[t % 2, i], dgu_h.at[i, rows, cols], dgu_out.at[t % 2, i]) for i in (0, 1)]

    def dgu_read(number, slot):
        rows = pl.ds(pl.multiple_of(number * DTOK, DTOK), DTOK)
        return [pltpu.make_async_copy(dgu_h.at[i, rows, :], IN.at[slot, i], dgu_in.at[slot, i]) for i in (0, 1)]

    def top_block(j, carry):
        for t in range(nt):
            tick(j, t, False)

            @pl.when(j == 0)
            def _():
                for c in tile_loads(t, a2_h, a2t_h, True):
                    c.wait()
                if t + 1 < nt:
                    for c in tile_loads(t + 1, a2_h, a2t_h, True):
                        c.start()
                else:
                    for c in weights[3:]:
                        c.start()

            @pl.when((j > 0) | (t > 1))
            def _():
                for c in dgu_write(j, t):
                    c.wait()
            tile_grads(1, j, t, lax.rem(j, SLOTS), refs, OUT.at[t % 2])
            for c in dgu_write(j, t):
                c.start()

            @pl.when(j == nj - 1)
            def _():
                h_load(t).start()
                tile_loads(t, a1_h, a1t_h, False)[1].start()
        finish(1, j)
        return carry

    lax.fori_loop(0, nj, top_block, 0)
    for t in (nt - 2, nt - 1):
        for c in dgu_write(nj - 1, t):
            c.wait()
    subs = tokens // DTOK // (PAUSE * nt)
    for v in range(2):
        for c in dgu_read(v, v):
            c.start()
    for c in weights[3:]:
        c.wait()
    for t in range(nt):
        h_load(t).wait()

    def between(i, t):
        for v in range(subs):
            number = ((i - nj) * nt + t) * subs + v
            slot = v % 2
            for c in dgu_read(number, slot):
                c.wait()
            da = mm_nt(IN[slot, 0], WG[1]) + mm_nt(IN[slot, 1], WU[1])
            through_norm(pl.ds(pl.multiple_of(number * DTOK, DTOK), DTOK), da, A, D, DT)

            @pl.when(number + 2 < tokens // DTOK)
            def _(number=number, slot=slot):
                for c in dgu_read(number + 2, slot):
                    c.start()

    def low_block(i, carry):
        low = i - nj - PAUSE
        for t in range(nt):
            tick(i, t, True)

            @pl.when(low < 0)
            def _():
                between(i, t)

            @pl.when((low >= 0) & (low < nj))
            def _():
                @pl.when(low == 0)
                def _():
                    for c in tile_loads(t, a1_h, a1t_h, False):
                        c.wait()
                tile_grads(0, low, t, lax.rem(i - PAUSE, SLOTS), refs)

        for p in range(PAUSE):
            @pl.when(i == nj + p)
            def _():
                for t in range(p * nt // PAUSE, (p + 1) * nt // PAUSE):
                    tile_loads(t, a1_h, a1t_h, False)[0].start()

        @pl.when((low >= 0) & (low < nj))
        def _():
            finish(0, low)
        return carry

    last = 2 * nj + PAUSE + max(nt + steps[-1][2], 1 + 2 * (streams - 1) + steps[-1][2]) // nt
    lax.fori_loop(nj, last + 1, low_block, 0)

    for c in (2 * nj - 2, 2 * nj - 1):
        place, j = c % 2, c % nj
        cols = slice(j * COLS, (j + 1) * COLS)
        for i, o in enumerate((mg_o, mu_o, vg_o, vu_o)):
            pltpu.make_async_copy(MV.at[place, i // 2, (i % 2) * half : (i % 2 + 1) * half], o.at[0, :, cols], mv_out.at[place, i]).wait()
        for i, o in enumerate((wg_o, wu_o)):
            pltpu.make_async_copy(NEW.at[c, :, i * half : (i + 1) * half], o.at[0, :, :, cols], out_sem.at[place, i]).wait()
    for k in range(streams):
        cols = slice(k * WIDE, (k + 1) * WIDE)
        for i, o in enumerate((md_o, vd_o)):
            pltpu.make_async_copy(MVD.at[k, i], o.at[0, :, cols], mvd_out.at[k, i]).wait()
        pltpu.make_async_copy(NEWD.at[0, k], wd_o.at[0, :, :, cols], outd_sem.at[k]).wait()


def grads(n, *args):
    a1, wg, wd = args[1], args[7], args[9]
    tokens, d = a1.shape
    layers, _, ff = wg.shape
    nj, nt, hops, streams = ff // COLS, tokens // TOK, n // 2, d // WIDE
    half, down = d // n, ff // n
    any_ = pl.BlockSpec(memory_space=pl.ANY)
    dma = pltpu.SemaphoreType.DMA
    own = [jax.ShapeDtypeStruct((layers, half, ff), F32)] * 2 + [jax.ShapeDtypeStruct((layers, down, d), F32)]
    return pl.pallas_call(
        functools.partial(grads_kernel, n),
        in_specs=[any_] * len(args),
        out_specs=[any_] * 10,
        out_shape=[jax.ShapeDtypeStruct((layers, n, half, ff), BF)] * 2 + [jax.ShapeDtypeStruct((layers, n, down, d), BF)] + own + own + [jax.ShapeDtypeStruct((2, tokens, ff), BF)],
        scratch_shapes=[
            pltpu.VMEM((tokens, d), BF), pltpu.VMEM((d, tokens), BF), pltpu.VMEM((tokens, d), BF), pltpu.VMEM((d, tokens), BF),
            pltpu.VMEM((layers * ff, d), F32),
            pltpu.VMEM((layers, d, ff), BF), pltpu.VMEM((layers, d, ff), BF), pltpu.VMEM((layers, ff, d), BF),
            pltpu.VMEM((SLOTS, n, 2 * half, COLS), F32), pltpu.VMEM((d, COLS), F32),
            pltpu.VMEM((layers * nj, n, 2 * half, COLS), BF), pltpu.VMEM((layers, streams, n, down, WIDE), BF),
            pltpu.VMEM((SLOTS, 2, hops, 2 * half, COLS), BF),
            pltpu.VMEM((streams, 2, hops, down, WIDE), BF),
            pltpu.VMEM((2, 2, 2 * half, COLS), F32), pltpu.VMEM((streams, 2, down, WIDE), F32),
            pltpu.VMEM((2, 2, TOK, COLS), BF), pltpu.VMEM((2, 2, DTOK, ff), BF),
            dma((nt, 4)), dma((2, 3)), dma((nt,)), dma((4, SLOTS, 2, hops)), dma((4, streams, 2, hops)),
            dma((2, 4)), dma((2, 4)), dma((streams, 2)), dma((streams, 2)), dma((2, 2)), dma((streams,)), dma((2, 2)), dma((2, 2)),
        ],
        compiler_params=pltpu.CompilerParams(vmem_limit_bytes=VMEM_LIMIT, collective_id=0, has_side_effects=True),
        name="grads",
    )(*args)[:9]


def solution(mesh):
    n = mesh.shape["dp"]

    def step(x, dy, wg, wu, wd, mg, mu, md, vg, vu, vd):
        a1, a1t, a2, a2t, h, dyt = forward(x, dy, wg, wu, wd)
        out = grads(n, dy, a1, a1t, a2, a2t, h, dyt, wg, wu, wd, mg, mu, md, vg, vu, vd)
        return tuple(t.reshape(t.shape[0], -1, t.shape[-1]) for t in out)

    data, whole, own = P(("rep", "dp"), None, None), P(), P(None, "dp", None)
    return jax.shard_map(
        step, mesh=mesh, in_specs=(data,) * 2 + (whole,) * 3 + (own,) * 6,
        out_specs=(P("rep", None, None),) * 3 + (P("rep", "dp", None),) * 6, check_vma=False,
    )
```

```python
import functools

import jax
import jax.numpy as jnp
from jax import lax
from jax.experimental import pallas as pl
from jax.experimental.pallas import tpu as pltpu
from jax.sharding import PartitionSpec as P

BF = jnp.bfloat16
F32 = jnp.float32
TILE = 512
TOK = 1024
COLS = 256
WIDE = 256
DTOK = 256
PAUSE = 2
SLOTS = 3
MESH = pl.DeviceIdType.MESH
VMEM_LIMIT = 67043328


def mm(a, b):
    return jnp.dot(a, b, preferred_element_type=F32)


def mm_nt(a, b):
    return lax.dot_general(a, b, (((1,), (1,)), ((), ())), preferred_element_type=F32)


def normed(h):
    wide = h.astype(F32)
    scale = lax.rsqrt(jnp.mean(wide * wide, -1, keepdims=True) + 1e-6)
    return (wide * scale).astype(BF)


def forward_kernel(x_ref, dy_ref, wg_ref, wu_ref, wd_ref, a1_ref, a1t_ref, a2_ref, a2t_ref, h_ref, dyt_ref):
    x = x_ref[0]
    a = normed(x)
    a1_ref[...] = a
    a1t_ref[...] = a.T
    dyt_ref[...] = dy_ref[0].T
    total = None
    for j in range(wg_ref.shape[2] // COLS):
        cols = slice(j * COLS, (j + 1) * COLS)
        gate = mm(a, wg_ref[0, :, cols])
        up = mm(a, wu_ref[0, :, cols])
        act = (gate * jax.nn.sigmoid(gate) * up).astype(BF)
        part = mm(act, wd_ref[0, cols, :])
        total = part if total is None else total + part
    h = (x.astype(F32) + total.astype(BF).astype(F32)).astype(BF)
    h_ref[...] = h
    a2 = normed(h)
    a2_ref[...] = a2
    a2t_ref[...] = a2.T


def forward(x, dy, wg, wu, wd):
    _, tokens, d = x.shape
    ff = wg.shape[2]
    row = pl.BlockSpec((1, TILE, d), lambda i: (0, i, 0))
    out = pl.BlockSpec((TILE, d), lambda i: (i, 0))
    out_t = pl.BlockSpec((d, TILE), lambda i: (0, i))
    w_in = pl.BlockSpec((1, d, ff), lambda i: (0, 0, 0))
    w_out = pl.BlockSpec((1, ff, d), lambda i: (0, 0, 0))
    straight, turned = jax.ShapeDtypeStruct((tokens, d), BF), jax.ShapeDtypeStruct((d, tokens), BF)
    return pl.pallas_call(
        forward_kernel,
        grid=(tokens // TILE,),
        in_specs=[row, row, w_in, w_in, w_out],
        out_specs=[out, out_t, out, out_t, out, out_t],
        out_shape=[straight, turned, straight, turned, straight, turned],
        compiler_params=pltpu.CompilerParams(vmem_limit_bytes=VMEM_LIMIT, dimension_semantics=("arbitrary",)),
        name="forward",
    )(x, dy, wg, wu, wd)


def tile_grads(layer, j, t, slot, refs, keep=None):
    A, AT, D, DT, WG, WU, WD, GU, DWT = refs
    rows = slice(t * TOK, (t + 1) * TOK)
    cols = pl.ds(pl.multiple_of(j * COLS, COLS), COLS)
    wg, wu = WG[layer, :, cols], WU[layer, :, cols]
    a, dy = A[rows, :], D[rows, :]
    gate, up = mm(a, wg), mm(a, wu)
    dact = mm_nt(dy, WD[layer, cols, :]).astype(BF).astype(F32)
    sig = jax.nn.sigmoid(gate)
    silu = gate * sig
    act = (silu * up).astype(BF)
    dup = (dact * silu).astype(BF)
    dgate = (dact * up * (sig + silu * (1.0 - sig))).astype(BF)
    if keep is not None:
        keep[0] = dgate
        keep[1] = dup
    at, dt = AT[:, rows], DT[:, rows]
    _, n, rows_of, _ = GU.shape
    half = rows_of // 2
    dwt = mm(dt, act)
    dwg = mm(at, dgate).reshape(n, half, COLS)
    dwu = mm(at, dup).reshape(n, half, COLS)
    if t == 0:
        DWT[...] = dwt
        GU[slot, :, :half, :] = dwg
        GU[slot, :, half:, :] = dwu
    else:
        DWT[...] += dwt
        GU[slot, :, :half, :] += dwg
        GU[slot, :, half:, :] += dwu


def through_norm(rows, da, A, D, DT):
    h = A[rows, :].astype(F32)
    s = lax.rsqrt(jnp.mean(h * h, -1, keepdims=True) + 1e-6)
    da = da.astype(BF).astype(F32)
    dh = da * s - h * (s * s * s * jnp.mean(da * h, -1, keepdims=True))
    dh = (D[rows, :].astype(F32) + dh.astype(BF).astype(F32)).astype(BF)
    D[rows, :] = dh
    DT[:, rows] = dh.T


def adamw(w, m, v, g):
    m = 0.9 * m + 0.1 * g
    v = 0.95 * v + 0.05 * g * g
    step = m * lax.rsqrt(v + 1e-8) + 0.1 * w
    return (w - 0.02 * step).astype(BF), m, v


class Ring:
    def __init__(self, n, me, got, sems):
        self.n, self.me, self.hops = n, me, n // 2
        self.to = (lax.rem(me + n - 1, n), lax.rem(me + 1, n))
        self.got = got
        self.sum_out, self.sum_in, self.new_out, self.new_in = sems

    def owner(self, way, distance):
        return lax.rem(self.me + (self.n - distance if way == 0 else distance), self.n)

    def part(self, way, half_only):
        rows = self.got.shape[2]
        if not half_only:
            return slice(0, rows)
        return slice(0, rows // 2) if way == 0 else slice(rows // 2, rows)

    def sum_copy(self, way, step):
        part = self.part(way, step == 0)
        source = self.got.at[way, self.hops - 1, part] if step == 0 else self.got.at[way, step - 1]
        return pltpu.make_async_remote_copy(
            source, self.got.at[way, step, part], self.sum_out.at[way, step], self.sum_in.at[way, step],
            device_id={"dp": self.to[way]}, device_id_type=MESH,
        )

    def new_copy(self, way, step, new):
        part = self.part(way, step == self.hops - 1)
        block = new.at[self.owner(1 - way, step), part]
        return pltpu.make_async_remote_copy(
            block, block, self.new_out.at[way, step], self.new_in.at[way, step],
            device_id={"dp": self.to[way]}, device_id_type=MESH,
        )

    def arrived(self, way, step, new):
        part = self.part(way, step == self.hops - 1)
        block = new.at[self.owner(1 - way, step + 1), part]
        return pltpu.make_async_remote_copy(
            block, block, self.new_out.at[way, step], self.new_in.at[way, step],
            device_id={"dp": self.to[way]}, device_id_type=MESH,
        )

    def sum_step(self, step, local):
        for way in (0, 1):
            if step:
                before = self.sum_copy(way, step - 1)
                before.wait_send()
                before.wait_recv()
        for way in (0, 1):
            term = local(self.owner(way, self.hops - step))
            if step == 0:
                self.got[way, self.hops - 1, self.part(way, True)] = term[self.part(way, True)].astype(BF)
            elif step == 1:
                mine, other = self.part(way, True), self.part(1 - way, True)
                got = self.got[way, 0, mine].astype(F32)
                self.got[way, 0, mine] = (got + term[mine]).astype(BF)
                self.got[way, 0, other] = term[other].astype(BF)
            else:
                self.got[way, step - 1] = (self.got[way, step - 1].astype(F32) + term).astype(BF)
        for way in (0, 1):
            self.sum_copy(way, step).start()

    def total(self, local):
        for way in (0, 1):
            before = self.sum_copy(way, self.hops - 1)
            before.wait_send()
            before.wait_recv()
        total = local(self.me) + self.got[0, self.hops - 1].astype(F32) + self.got[1, self.hops - 1].astype(F32)
        return total.astype(BF).astype(F32)

    def new_step(self, step, new):
        for way in (0, 1):
            if step:
                self.new_copy(way, step - 1, new).wait_send()
                self.arrived(way, step - 1, new).wait_recv()
        if step < self.hops:
            for way in (0, 1):
                self.new_copy(way, step, new).start()


def grads_kernel(
    n, dy_h, a1_h, a1t_h, a2_h, a2t_h, h_h, dyt_h, wg_h, wu_h, wd_h, mg_h, mu_h, md_h, vg_h, vu_h, vd_h,
    wg_o, wu_o, wd_o, mg_o, mu_o, md_o, vg_o, vu_o, vd_o, dgu_h,
    A, AT, D, DT, S, WG, WU, WD, GU, DWT, NEW, NEWD, GOT, GOTD, MV, MVD, OUT, IN,
    load, wsem, hsem, ring_sem, ringd_sem, mv_in, mv_out, mvd_in, mvd_out, out_sem, outd_sem, dgu_out, dgu_in,
):
    me = lax.axis_index("dp")
    left, right = lax.rem(me + n - 1, n), lax.rem(me + 1, n)
    barrier = pltpu.get_barrier_semaphore()
    for neighbour in (left, right):
        pl.semaphore_signal(barrier, inc=1, device_id={"dp": neighbour}, device_id_type=MESH)

    tokens, d = A.shape
    nt = tokens // TOK
    ff = WG.shape[2]
    nj = ff // COLS
    half, down = d // n, ff // n
    hops = n // 2
    streams = d // WIDE

    def tile_loads(t, a_h, at_h, with_dy):
        rows = slice(t * TOK, (t + 1) * TOK)
        pairs = [(a_h.at[rows, :], A.at[rows, :]), (at_h.at[:, rows], AT.at[:, rows])]
        if with_dy:
            pairs += [(dy_h.at[0, rows, :], D.at[rows, :]), (dyt_h.at[:, rows], DT.at[:, rows])]
        return [pltpu.make_async_copy(s, o, load.at[t, i]) for i, (s, o) in enumerate(pairs)]

    def h_load(t):
        rows = slice(t * TOK, (t + 1) * TOK)
        return pltpu.make_async_copy(h_h.at[rows, :], A.at[rows, :], hsem.at[t])

    weights = [
        pltpu.make_async_copy(s.at[l], o.at[l], wsem.at[l, i])
        for l in (1, 0) for i, (s, o) in enumerate(((wg_h, WG), (wu_h, WU), (wd_h, WD)))
    ]
    for c in weights[:3]:
        c.start()
    for c in tile_loads(0, a2_h, a2t_h, True):
        c.start()
    for c in weights[:3]:
        c.wait()
    pl.semaphore_wait(barrier, 2)

    refs = (A, AT, D, DT, WG, WU, WD, GU, DWT)

    def gate_up(c, op, step):
        slot, layer, j = lax.rem(c, SLOTS), 1 - c // nj, lax.rem(c, nj)
        ring = Ring(n, me, GOT.at[slot], [ring_sem.at[k, slot] for k in range(4)])
        new = NEW.at[c]
        cols = pl.ds(pl.multiple_of(j * COLS, COLS), COLS)
        place = lax.rem(c, 2)

        def local(device):
            return GU[slot, device]

        def moments(m_g, m_u, v_g, v_u):
            return [
                (m_g.at[layer, :, cols], MV.at[place, 0, :half]), (m_u.at[layer, :, cols], MV.at[place, 0, half:]),
                (v_g.at[layer, :, cols], MV.at[place, 1, :half]), (v_u.at[layer, :, cols], MV.at[place, 1, half:]),
            ]

        fetch = lambda: [pltpu.make_async_copy(a, b, mv_in.at[place, i]) for i, (a, b) in enumerate(moments(mg_h, mu_h, vg_h, vu_h))]
        keep = lambda: [pltpu.make_async_copy(b, a, mv_out.at[place, i]) for i, (a, b) in enumerate(moments(mg_o, mu_o, vg_o, vu_o))]
        write = lambda: [
            pltpu.make_async_copy(new.at[:, :half], wg_o.at[layer, :, :, cols], out_sem.at[place, 0]),
            pltpu.make_async_copy(new.at[:, half:], wu_o.at[layer, :, :, cols], out_sem.at[place, 1]),
        ]
        if op == "sum":
            if step == hops // 2:
                @pl.when(c >= 2)
                def _():
                    for copy in keep():
                        copy.wait()
                for copy in fetch():
                    copy.start()
            ring.sum_step(step, local)
        elif op == "update":
            for copy in fetch():
                copy.wait()
            g = ring.total(local)
            own = pl.ds(pl.multiple_of(me * half, half), half)
            for i, w in enumerate((WG, WU)):
                rows = slice(i * half, (i + 1) * half)
                nw, m, v = adamw(w[layer, own, cols].astype(F32), MV[place, 0, rows], MV[place, 1, rows], g[rows])
                MV[place, 0, rows] = m
                MV[place, 1, rows] = v
                NEW[c, me, rows] = nw
            ring.new_step(0, new)
            for copy in keep():
                copy.start()
        else:
            ring.new_step(step, new)
            if step == hops:
                @pl.when(c >= 2)
                def _():
                    for copy in write():
                        copy.wait()
                for copy in write():
                    copy.start()

    def down_block(layer, k, op, step):
        ring = Ring(n, me, GOTD.at[k], [ringd_sem.at[i, k] for i in range(4)])
        new = NEWD.at[layer, k]
        cols = slice(k * WIDE, (k + 1) * WIDE)

        def local(device):
            return S[pl.ds(pl.multiple_of(layer * ff + device * down, 32), down), cols]

        fetch = lambda: [pltpu.make_async_copy(s.at[layer, :, cols], MVD.at[k, i], mvd_in.at[k, i]) for i, s in enumerate((md_h, vd_h))]
        keep = lambda: [pltpu.make_async_copy(MVD.at[k, i], o.at[layer, :, cols], mvd_out.at[k, i]) for i, o in enumerate((md_o, vd_o))]
        write = lambda: pltpu.make_async_copy(new, wd_o.at[layer, :, :, cols], outd_sem.at[k])
        if op == "sum":
            if step == hops // 2:
                @pl.when(layer == 0)
                def _():
                    for copy in keep():
                        copy.wait()
                for copy in fetch():
                    copy.start()
            ring.sum_step(step, local)
        elif op == "update":
            for copy in fetch():
                copy.wait()
            g = ring.total(local)
            own = pl.ds(pl.multiple_of(me * down, 32), down)
            nw, m, v = adamw(WD[layer, own, cols].astype(F32), MVD[k, 0], MVD[k, 1], g)
            MVD[k, 0] = m
            MVD[k, 1] = v
            NEWD[layer, k, me] = nw
            ring.new_step(0, new)
            for copy in keep():
                copy.start()
        else:
            ring.new_step(step, new)
            if step == hops:
                @pl.when(layer == 0)
                def _():
                    write().wait()
                write().start()

    steps = [("sum", s, 2 * s) for s in range(hops)] + [("update", 0, 2 * hops)]
    steps += [("new", s, 2 * hops + 1 + 2 * s) for s in range(1, hops + 1)]

    def tick(i, t, with_down):
        for op, step, after in steps:
            ago, at_tick = divmod(after, nt)
            if at_tick == t:
                x = i - 1 - ago

                @pl.when(((x >= 0) & (x < nj)) | ((x >= nj + PAUSE) & (x < 2 * nj + PAUSE)))
                def _(x=x, op=op, step=step):
                    gate_up(x - PAUSE * (x // (nj + PAUSE)), op, step)
        if with_down:
            for k in range(streams):
                for op, step, after in steps:
                    ago, at_tick = divmod(after + 1 + 2 * k, nt)
                    if at_tick == t:
                        ready = i - ago

                        @pl.when((ready == nj) | (ready == 2 * nj + PAUSE))
                        def _(ready=ready, op=op, step=step, k=k):
                            down_block(2 - ready // nj, k, op, step)

    def finish(layer, j):
        S[pl.ds(pl.multiple_of(layer * ff + j * COLS, COLS), COLS), :] = DWT[...].T

    def dgu_write(j, t):
        rows = slice(t * TOK, (t + 1) * TOK)
        cols = pl.ds(pl.multiple_of(j * COLS, COLS), COLS)
        return [pltpu.make_async_copy(OUT.at[t % 2, i], dgu_h.at[i, rows, cols], dgu_out.at[t % 2, i]) for i in (0, 1)]

    def dgu_read(number, slot):
        rows = pl.ds(pl.multiple_of(number * DTOK, DTOK), DTOK)
        return [pltpu.make_async_copy(dgu_h.at[i, rows, :], IN.at[slot, i], dgu_in.at[slot, i]) for i in (0, 1)]

    def top_block(j, carry):
        for t in range(nt):
            tick(j, t, False)

            @pl.when(j == 0)
            def _():
                for c in tile_loads(t, a2_h, a2t_h, True):
                    c.wait()
                if t + 1 < nt:
                    for c in tile_loads(t + 1, a2_h, a2t_h, True):
                        c.start()
                else:
                    for c in weights[3:]:
                        c.start()

            @pl.when((j > 0) | (t > 1))
            def _():
                for c in dgu_write(j, t):
                    c.wait()
            tile_grads(1, j, t, lax.rem(j, SLOTS), refs, OUT.at[t % 2])
            for c in dgu_write(j, t):
                c.start()

            @pl.when(j == nj - 1)
            def _():
                h_load(t).start()
                tile_loads(t, a1_h, a1t_h, False)[1].start()
        finish(1, j)
        return carry

    lax.fori_loop(0, nj, top_block, 0)
    for t in (nt - 2, nt - 1):
        for c in dgu_write(nj - 1, t):
            c.wait()
    subs = tokens // DTOK // (PAUSE * nt)
    for v in range(2):
        for c in dgu_read(v, v):
            c.start()
    for c in weights[3:]:
        c.wait()
    for t in range(nt):
        h_load(t).wait()

    def between(i, t):
        for v in range(subs):
            number = ((i - nj) * nt + t) * subs + v
            slot = v % 2
            for c in dgu_read(number, slot):
                c.wait()
            da = mm_nt(IN[slot, 0], WG[1]) + mm_nt(IN[slot, 1], WU[1])
            through_norm(pl.ds(pl.multiple_of(number * DTOK, DTOK), DTOK), da, A, D, DT)

            @pl.when(number + 2 < tokens // DTOK)
            def _(number=number, slot=slot):
                for c in dgu_read(number + 2, slot):
                    c.start()

    def low_block(i, carry):
        low = i - nj - PAUSE
        for t in range(nt):
            tick(i, t, True)

            @pl.when(low < 0)
            def _():
                between(i, t)

            @pl.when((low >= 0) & (low < nj))
            def _():
                @pl.when(low == 0)
                def _():
                    for c in tile_loads(t, a1_h, a1t_h, False):
                        c.wait()
                tile_grads(0, low, t, lax.rem(i - PAUSE, SLOTS), refs)

        for p in range(PAUSE):
            @pl.when(i == nj + p)
            def _():
                for t in range(p * nt // PAUSE, (p + 1) * nt // PAUSE):
                    tile_loads(t, a1_h, a1t_h, False)[0].start()

        @pl.when((low >= 0) & (low < nj))
        def _():
            finish(0, low)
        return carry

    last = 2 * nj + PAUSE + max(nt + steps[-1][2], 1 + 2 * (streams - 1) + steps[-1][2]) // nt
    lax.fori_loop(nj, last + 1, low_block, 0)

    for c in (2 * nj - 2, 2 * nj - 1):
        place, j = c % 2, c % nj
        cols = slice(j * COLS, (j + 1) * COLS)
        for i, o in enumerate((mg_o, mu_o, vg_o, vu_o)):
            pltpu.make_async_copy(MV.at[place, i // 2, (i % 2) * half : (i % 2 + 1) * half], o.at[0, :, cols], mv_out.at[place, i]).wait()
        for i, o in enumerate((wg_o, wu_o)):
            pltpu.make_async_copy(NEW.at[c, :, i * half : (i + 1) * half], o.at[0, :, :, cols], out_sem.at[place, i]).wait()
    for k in range(streams):
        cols = slice(k * WIDE, (k + 1) * WIDE)
        for i, o in enumerate((md_o, vd_o)):
            pltpu.make_async_copy(MVD.at[k, i], o.at[0, :, cols], mvd_out.at[k, i]).wait()
        pltpu.make_async_copy(NEWD.at[0, k], wd_o.at[0, :, :, cols], outd_sem.at[k]).wait()


def grads(n, *args):
    a1, wg, wd = args[1], args[7], args[9]
    tokens, d = a1.shape
    layers, _, ff = wg.shape
    nj, nt, hops, streams = ff // COLS, tokens // TOK, n // 2, d // WIDE
    half, down = d // n, ff // n
    any_ = pl.BlockSpec(memory_space=pl.ANY)
    dma = pltpu.SemaphoreType.DMA
    own = [jax.ShapeDtypeStruct((layers, half, ff), F32)] * 2 + [jax.ShapeDtypeStruct((layers, down, d), F32)]
    return pl.pallas_call(
        functools.partial(grads_kernel, n),
        in_specs=[any_] * len(args),
        out_specs=[any_] * 10,
        out_shape=[jax.ShapeDtypeStruct((layers, n, half, ff), BF)] * 2 + [jax.ShapeDtypeStruct((layers, n, down, d), BF)] + own + own + [jax.ShapeDtypeStruct((2, tokens, ff), BF)],
        scratch_shapes=[
            pltpu.VMEM((tokens, d), BF), pltpu.VMEM((d, tokens), BF), pltpu.VMEM((tokens, d), BF), pltpu.VMEM((d, tokens), BF),
            pltpu.VMEM((layers * ff, d), F32),
            pltpu.VMEM((layers, d, ff), BF), pltpu.VMEM((layers, d, ff), BF), pltpu.VMEM((layers, ff, d), BF),
            pltpu.VMEM((SLOTS, n, 2 * half, COLS), F32), pltpu.VMEM((d, COLS), F32),
            pltpu.VMEM((layers * nj, n, 2 * half, COLS), BF), pltpu.VMEM((layers, streams, n, down, WIDE), BF),
            pltpu.VMEM((SLOTS, 2, hops, 2 * half, COLS), BF),
            pltpu.VMEM((streams, 2, hops, down, WIDE), BF),
            pltpu.VMEM((2, 2, 2 * half, COLS), F32), pltpu.VMEM((streams, 2, down, WIDE), F32),
            pltpu.VMEM((2, 2, TOK, COLS), BF), pltpu.VMEM((2, 2, DTOK, ff), BF),
            dma((nt, 4)), dma((2, 3)), dma((nt,)), dma((4, SLOTS, 2, hops)), dma((4, streams, 2, hops)),
            dma((2, 4)), dma((2, 4)), dma((streams, 2)), dma((streams, 2)), dma((2, 2)), dma((streams,)), dma((2, 2)), dma((2, 2)),
        ],
        compiler_params=pltpu.CompilerParams(vmem_limit_bytes=VMEM_LIMIT, collective_id=0, has_side_effects=True),
        name="grads",
    )(*args)[:9]


def place_kernel(count, *refs):
    ins, outs, held, (arrive, leave) = refs[:count], refs[count : 2 * count], refs[2 * count : 3 * count], refs[3 * count :]
    pieces = [(i, l) for i in range(count) for l in range(ins[i].shape[0])]
    loads = [pltpu.make_async_copy(ins[i].at[l], held[i].at[l], arrive.at[i, l]) for i, l in pieces]
    stores = [pltpu.make_async_copy(held[i].at[l], outs[i].at[l], leave.at[i, l]) for i, l in pieces]
    for copy in loads:
        copy.start()
    for load, store in zip(loads, stores, strict=True):
        load.wait()
        store.start()
    for store in stores:
        store.wait()


def place(arrays):
    count, layers = len(arrays), arrays[0].shape[0]
    any_ = pl.BlockSpec(memory_space=pl.ANY)
    return pl.pallas_call(
        functools.partial(place_kernel, count),
        in_specs=[any_] * count,
        out_specs=[any_] * count,
        out_shape=[jax.ShapeDtypeStruct(t.shape, t.dtype) for t in arrays],
        scratch_shapes=[pltpu.VMEM(t.shape, t.dtype) for t in arrays] + [pltpu.SemaphoreType.DMA((count, layers))] * 2,
        compiler_params=pltpu.CompilerParams(vmem_limit_bytes=VMEM_LIMIT),
        name="place",
    )(*arrays)


def solution(mesh):
    n = mesh.shape["dp"]

    def step(x, dy, wg, wu, wd, mg, mu, md, vg, vu, vd):
        a1, a1t, a2, a2t, h, dyt = forward(x, dy, wg, wu, wd)
        out = grads(n, dy, a1, a1t, a2, a2t, h, dyt, wg, wu, wd, mg, mu, md, vg, vu, vd)
        return tuple(place([t.reshape(t.shape[0], -1, t.shape[-1]) for t in out]))

    data, whole, own = P(("rep", "dp"), None, None), P(), P(None, "dp", None)
    return jax.shard_map(
        step, mesh=mesh, in_specs=(data,) * 2 + (whole,) * 3 + (own,) * 6,
        out_specs=(P("rep", None, None),) * 3 + (P("rep", "dp", None),) * 6, check_vma=False,
    )
```
